32 devices in a mesh: vp: 8 (over z, y), rep: 4 (over x, core).
Axes of the slice: x: 2, y: 2, z: 4, core: 2. Of those that a mesh axis runs over, the one named last changes fastest.
Arguments:
- features: bfloat16 [65536, 256], P(('vp', 'rep')), may hold values from -48 to 48
- tile_values: bfloat16 [8192, 128, 128], P(('vp', 'rep')), may hold values from 0 to 0.0014648438
- tile_cols: int32 [8192], P(('vp', 'rep')), may hold values from 0 to 31, as said below
- halo_rows: int32 [32, 4, 4], P(('vp', 'rep')), may hold values from 0 to 15
Outputs:
- scores: bfloat16 [65536, 256], P(('vp', 'rep'))
The draws below stay inside these ranges and needn't reach their ends.
Inputs may be any that keep to these rules, and one draw needn't show every extreme that they name: `tile_cols`: values below 16 name one of the shard's own row blocks; value 16 + o * 4 + j names the j-th block sent by peer o. Every value occurs on every shard.
All inputs are finite; a program needn't handle non-finite values.
Results may differ from the reference program's by a relative error of at most 0.002.
Values may be sent and summed in bfloat16 or wider, within the bound.
A program may use at most 128 MiB of HBM per device.

```python
import math
import jax
import jax.numpy as jnp
from jax import lax

CLASSES = 256
TILE = 128
BLOCKS_DEV = 16
TILES_ROW = 16
HALO_SLOTS = 4
ITERS = 3
SHARDS = 32
VERTICES = 65536
TILES = 8192


def draw_features(key, part):
    scale_key, noise_key, common_key = jax.random.split(key, 3)
    block_count = SHARDS * BLOCKS_DEV
    scales = jnp.exp(jax.random.uniform(scale_key, (block_count, 1, 1), minval=0.0, maxval=math.log(8.0)))
    noise = jnp.clip(jax.random.normal(noise_key, (block_count, TILE, CLASSES)), -6.0, 6.0)
    values = scales * noise
    values = jnp.clip(values, -48.0, 48.0).reshape(block_count * TILE, CLASSES)
    return values.astype(jnp.bfloat16)


def draw_tile_cols(key, part):
    slot_count = BLOCKS_DEV + 4 * HALO_SLOTS
    per_device = BLOCKS_DEV * TILES_ROW
    device_keys = jax.random.split(key, SHARDS)

    def one_device(device_key):
        first_key, second_key = jax.random.split(device_key)
        base_slots = jax.random.randint(first_key, (per_device,), 0, slot_count, dtype=jnp.int32)
        placing = jax.random.permutation(second_key, per_device)
        return base_slots.at[placing[:slot_count]].set(jnp.arange(slot_count, dtype=jnp.int32))
    return jax.vmap(one_device)(device_keys).reshape(-1)


def with_ends(entries, key, least, top_value):
    index_at = [jax.random.randint(jax.random.fold_in(key, axis), (), 0, length) for axis, length in enumerate(entries.shape)]
    main_axis = entries.shape.index(max(entries.shape))
    next_to = index_at[:main_axis] + [(index_at[main_axis] + 1) % entries.shape[main_axis]] + index_at[main_axis + 1:]
    return entries.at[tuple(index_at)].set(least).at[tuple(next_to)].set(top_value)


def levels(key, extent, cuts, least, largest):
    gain, own = 1.0, jax.random.fold_in(key, 6)
    for dim, parts in cuts:
        heights = jnp.exp(jax.random.uniform(jax.random.fold_in(own, dim), (parts,), jnp.float32, least / len(cuts), largest / len(cuts)))
        gain = gain * jnp.repeat(heights, extent[dim] // parts).reshape([-1 if axis == dim else 1 for axis in range(len(extent))])
    return gain


def setup_inputs(seed: int = 0) -> dict:
    seeds = jax.random.split(jax.random.key(seed), 5)
    return {
        "features": draw_features(jax.random.fold_in(seeds[4], 71), 0),
        "tile_values": jnp.clip(0.0014648438 * jax.random.uniform(seeds[1], (TILES, TILE, TILE), jnp.float32) ** levels(seeds[1], (TILES, TILE, TILE), ((0, 32),), -0.2, 0.2), 0.0, 0.0014648438).astype(jnp.bfloat16),
        "tile_cols": draw_tile_cols(jax.random.fold_in(seeds[4], 71), 0),
        "halo_rows": with_ends(jax.random.randint(seeds[3], (SHARDS, 4, HALO_SLOTS), 0, BLOCKS_DEV), jax.random.fold_in(seeds[3], 1), 0, BLOCKS_DEV - 1).astype(jnp.int32),
    }


def reference(features, tile_values, tile_cols, halo_rows):
    nblocks = BLOCKS_DEV
    tiles_dev = BLOCKS_DEV * TILES_ROW
    device_ids = jnp.arange(SHARDS, dtype=jnp.int32)
    slots = tile_cols.reshape(SHARDS, tiles_dev).astype(jnp.int32)
    is_local = slots < nblocks
    halo_slot = jnp.maximum(slots - nblocks, 0)
    offset_slot = (halo_slot // HALO_SLOTS).astype(jnp.int32)
    slot_entry = (halo_slot % HALO_SLOTS).astype(jnp.int32)
    shift_by = jnp.array([1, -1, 4, -4], dtype=jnp.int32)[offset_slot]
    sender = ((device_ids[:, None] - shift_by) % SHARDS).astype(jnp.int32)
    sent_block = halo_rows[sender, offset_slot, slot_entry].astype(jnp.int32)
    source_block = jnp.where(is_local, device_ids[:, None] * nblocks + slots, sender * nblocks + sent_block).astype(jnp.int32)
    source_block = source_block.reshape(SHARDS, nblocks, TILES_ROW)
    tiles = tile_values.reshape(SHARDS, nblocks, TILES_ROW, TILE, TILE)
    teleport_part = 0.1 * features.astype(jnp.float32)
    current = features
    for iteration in range(ITERS):
        blocks = current.reshape(SHARDS * nblocks, TILE, CLASSES)

        def propagate_device(pair):
            tiles_here, sources_here = pair
            gathered = blocks[sources_here]
            return jnp.einsum('rtij,rtjc->ric', tiles_here.astype(jnp.float32), gathered.astype(jnp.float32), precision=lax.Precision.HIGHEST)
        propagated = lax.map(propagate_device, (tiles, source_block)).reshape(VERTICES, CLASSES)
        blended = 0.9 * propagated + teleport_part
        total_mass = lax.optimization_barrier(jnp.sum(blended * blended, axis=0))
        current = (blended / jnp.sqrt(0.05 + total_mass / VERTICES)).astype(jnp.bfloat16)
    return current
```

```python
import functools

import jax
import jax.numpy as jnp
from jax import lax
from jax.experimental import pallas as pl
from jax.experimental.pallas import tpu as pltpu
from jax.sharding import PartitionSpec as P

ITERS = 3
LANES = 128
OFFSETS = (1, -1, 4, -4)
MESH = pl.DeviceIdType.MESH
LOADS = 8


def kernel(vp_count, rep_count, vertices, slots, halves, *refs):
    cols_ref, rows_ref, feat_hbm, tiles_hbm, out_hbm = refs[:5]
    it_refs = iter(refs[5:])
    take = lambda count: [next(it_refs) for _ in range(count)]
    tiles = take(1)[0]
    tables = [take(halves) for _ in range(ITERS)]
    feats = take(halves)
    owns = take(halves)
    sends = [take(halves) for _ in range(ITERS)]
    finals = take(halves)
    stages = take(halves)
    mine_a = [take(halves) for _ in range(ITERS)]
    got_a = [take(halves) for _ in range(ITERS)]
    mine_b = [take(halves) for _ in range(ITERS)]
    got_b = [take(halves) for _ in range(ITERS)]
    (tile_sem, feat_sem, table_sem, out_sem, send_sem, recv_sem,
     a_send, a_recv, b_send, b_recv) = take(10)

    nblocks, tile_size = feats[0].shape[0], feats[0].shape[1]
    ntiles = tiles.shape[0]
    per_row = ntiles // nblocks
    my_vp, my_rep = lax.axis_index("vp"), lax.axis_index("rep")
    me = my_vp * rep_count + my_rep
    shards = vp_count * rep_count

    own_loads, table_loads = [], []
    for h in range(halves):
        part = feat_hbm.at[:, :, pl.ds(h * LANES, LANES)]
        own_loads.append(pltpu.make_async_copy(part, feats[h], feat_sem.at[h]))
        table_loads.append(
            pltpu.make_async_copy(part, tables[0][h].at[pl.ds(0, nblocks)], table_sem.at[h])
        )
    for h in range(halves):
        own_loads[h].start()
    for h in range(halves):
        table_loads[h].start()
    chunk = ntiles // LOADS
    tile_loads = []
    for k in range(LOADS):
        piece = pl.ds(k * chunk, chunk)
        tile_loads.append(pltpu.make_async_copy(tiles_hbm.at[piece], tiles.at[piece], tile_sem.at[k]))
        tile_loads[-1].start()

    peers = []
    for off in OFFSETS:
        flat = lax.rem(me + off + shards, shards)
        peers.append((flat // rep_count, lax.rem(flat, rep_count)))
    rep_peers = [(my_vp, lax.rem(my_rep + k, rep_count)) for k in range(1, rep_count)]
    vp_peers = [(lax.rem(my_vp + k, vp_count), my_rep) for k in range(1, vp_count)]
    everyone = peers + rep_peers + vp_peers
    barrier = pltpu.get_barrier_semaphore()
    for peer in everyone:
        pl.semaphore_signal(barrier, inc=1, device_id=peer, device_id_type=MESH)
    pl.semaphore_wait(barrier, len(everyone))

    def halo_copy(it, h, o):
        at = (it * halves + h) * 4 + o
        return pltpu.make_async_remote_copy(
            src_ref=sends[it][h].at[pl.ds(o * slots, slots)],
            dst_ref=tables[it][h].at[pl.ds(nblocks + o * slots, slots)],
            send_sem=send_sem.at[at],
            recv_sem=recv_sem.at[at],
            device_id=peers[o],
            device_id_type=MESH,
        )

    def send_halo(it, h, source):
        for k in range(4 * slots):
            sends[it][h][k] = source[rows_ref[k]]
        for o in (2, 3, 0, 1):
            halo_copy(it, h, o).start()

    def mass_copy(it, h, k, mine, got, s_sem, r_sem, group):
        at = (it * halves + h) * len(group) + k
        return pltpu.make_async_remote_copy(
            src_ref=mine[it][h],
            dst_ref=got[it][h].at[k],
            send_sem=s_sem.at[at],
            recv_sem=r_sem.at[at],
            device_id=group[k],
            device_id_type=MESH,
        )

    def copies_a(it, h):
        return [mass_copy(it, h, k, mine_a, got_a, a_send, a_recv, rep_peers) for k in range(len(rep_peers))]

    def copies_b(it, h):
        return [mass_copy(it, h, k, mine_b, got_b, b_send, b_recv, vp_peers) for k in range(len(vp_peers))]

    def mass_first(it, h, mass):
        mine_a[it][h][...] = mass
        for copy in copies_a(it, h):
            copy.start()

    def mass_second(it, h):
        for copy in copies_a(it, h):
            copy.wait_recv()
        mine_b[it][h][...] = mine_a[it][h][...] + jnp.sum(got_a[it][h][...], axis=0)
        for copy in copies_b(it, h):
            copy.start()

    def mass_total(it, h):
        for copy in copies_b(it, h):
            copy.wait_recv()
        total = mine_b[it][h][...] + jnp.sum(got_b[it][h][...], axis=0)
        return 1.0 / jnp.sqrt(0.05 + total / vertices)

    def propagate(it, h, gain):
        table = tables[it][h]

        def row(r, mass):
            first = r * per_row
            left = jnp.concatenate([tiles[first + t] for t in range(per_row)], axis=1)
            right = jnp.concatenate([table[cols_ref[first + t]] for t in range(per_row)], axis=0)
            total = jnp.dot(left, right, preferred_element_type=jnp.float32)
            blended = gain * total + 0.1 * feats[h][r].astype(jnp.float32)
            if it + 1 < ITERS:
                rounded = blended.astype(jnp.bfloat16)
                owns[h][r] = rounded
                tables[it + 1][h][r] = rounded
            else:
                finals[h][r] = blended
            squares = (blended * blended).reshape(tile_size // 8, 8, LANES)
            return mass + jnp.sum(squares, axis=0)

        mass = lax.fori_loop(0, nblocks, row, jnp.zeros((8, LANES), jnp.float32))
        return jnp.sum(mass, axis=0, keepdims=True)

    for h in range(halves):
        own_loads[h].wait()
        send_halo(0, h, feats[h])
    for h in range(halves):
        table_loads[h].wait()
    for load in tile_loads:
        load.wait()

    def finish(h):
        scale = mass_total(ITERS - 1, h)
        for b in range(nblocks):
            stages[h][b] = (finals[h][b] * scale).astype(jnp.bfloat16)
        pltpu.make_async_copy(
            stages[h], out_hbm.at[:, :, pl.ds(h * LANES, LANES)], out_sem.at[h]
        ).start()

    for it in range(ITERS):
        for h in range(halves):
            for o in range(4):
                halo_copy(it, h, o).wait_recv()
            gain = 0.9 if it == 0 else 0.9 * mass_total(it - 1, h)
            mass = propagate(it, h, gain)
            mass_first(it, h, mass)
            if it + 1 < ITERS:
                send_halo(it + 1, h, owns[h])
            mass_second(it, h)
    for h in range(halves):
        finish(h)
    for it in range(ITERS):
        for h in range(halves):
            for o in range(4):
                halo_copy(it, h, o).wait_send()
            for copy in copies_a(it, h) + copies_b(it, h):
                copy.wait_send()
    for h in range(halves):
        pltpu.make_async_copy(
            stages[h], out_hbm.at[:, :, pl.ds(h * LANES, LANES)], out_sem.at[h]
        ).wait()


def local(vp_count, rep_count, features, tile_values, tile_cols, halo_rows):
    tile_size = tile_values.shape[1]
    rows, classes = features.shape
    nblocks = rows // tile_size
    slots = halo_rows.shape[2]
    halves = classes // LANES
    shards = vp_count * rep_count
    block = (tile_size, LANES)
    bf16, f32 = jnp.bfloat16, jnp.float32
    each = ITERS * halves
    scratch = [pltpu.VMEM(tile_values.shape, bf16)]
    scratch += [pltpu.VMEM((nblocks + 4 * slots,) + block, bf16)] * each
    scratch += [pltpu.VMEM((nblocks,) + block, bf16)] * (2 * halves)
    scratch += [pltpu.VMEM((4 * slots,) + block, bf16)] * each
    scratch += [pltpu.VMEM((nblocks,) + block, f32)] * halves
    scratch += [pltpu.VMEM((nblocks,) + block, bf16)] * halves
    scratch += [pltpu.VMEM((1, LANES), f32)] * each
    scratch += [pltpu.VMEM((rep_count - 1, 1, LANES), f32)] * each
    scratch += [pltpu.VMEM((1, LANES), f32)] * each
    scratch += [pltpu.VMEM((vp_count - 1, 1, LANES), f32)] * each
    dma = lambda count: pltpu.SemaphoreType.DMA((count,))
    scratch += [dma(LOADS), dma(halves), dma(halves), dma(halves), dma(each * 4), dma(each * 4)]
    scratch += [dma(each * (rep_count - 1))] * 2 + [dma(each * (vp_count - 1))] * 2
    out = pl.pallas_call(
        functools.partial(kernel, vp_count, rep_count, rows * shards, slots, halves),
        out_shape=jax.ShapeDtypeStruct((nblocks, tile_size, classes), bf16),
        in_specs=[pl.BlockSpec(memory_space=pltpu.SMEM)] * 2
        + [pl.BlockSpec(memory_space=pl.ANY)] * 2,
        out_specs=pl.BlockSpec(memory_space=pl.ANY),
        scratch_shapes=scratch,
        compiler_params=pltpu.CompilerParams(
            collective_id=0, has_side_effects=True, vmem_limit_bytes=60 * 1024 * 1024
        ),
    )(tile_cols, halo_rows.reshape(-1), features.reshape(nblocks, tile_size, classes), tile_values)
    return out.reshape(rows, classes)


def solution(mesh):
    return jax.shard_map(
        functools.partial(local, mesh.shape["vp"], mesh.shape["rep"]),
        mesh=mesh,
        in_specs=(
            P(("vp", "rep"), None),
            P(("vp", "rep"), None, None),
            P(("vp", "rep")),
            P(("vp", "rep"), None, None),
        ),
        out_specs=P(("vp", "rep"), None),
        check_vma=False,
    )
```

```python
import functools

import jax
import jax.numpy as jnp
from jax import lax
from jax.experimental import pallas as pl
from jax.experimental.pallas import tpu as pltpu
from jax.sharding import PartitionSpec as P

ITERS = 3
LANES = 128
MESH = pl.DeviceIdType.MESH
LOADS = 8


def kernel(vp_count, rep_count, vertices, slots, halves, *refs):
    cols_ref, rows_ref, feat_hbm, tiles_hbm, out_hbm = refs[:5]
    it_refs = iter(refs[5:])
    take = lambda count: [next(it_refs) for _ in range(count)]
    tiles = take(1)[0]
    tables = [take(halves) for _ in range(ITERS)]
    feats = take(halves)
    owns = take(halves)
    sends = [take(halves) for _ in range(ITERS)]
    finals = take(halves)
    stages = take(halves)
    mine = [take(halves) for _ in range(ITERS)]
    got = [take(halves) for _ in range(ITERS)]
    order, place = take(2)
    (tile_sem, feat_sem, table_sem, out_sem, send_sem, recv_sem, mass_send, mass_recv) = take(8)

    nblocks, tile_size = feats[0].shape[0], feats[0].shape[1]
    ntiles = tiles.shape[0]
    per_row = ntiles // nblocks
    my_vp, my_rep = lax.axis_index("vp"), lax.axis_index("rep")
    me = my_vp * rep_count + my_rep
    shards = vp_count * rep_count

    own_loads, table_loads = [], []
    for h in range(halves):
        part = feat_hbm.at[:, :, pl.ds(h * LANES, LANES)]
        own_loads.append(pltpu.make_async_copy(part, feats[h], feat_sem.at[h]))
        table_loads.append(
            pltpu.make_async_copy(part, tables[0][h].at[pl.ds(0, nblocks)], table_sem.at[h])
        )
    for h in range(halves):
        own_loads[h].start()
    for h in range(halves):
        table_loads[h].start()
    chunk = ntiles // LOADS
    tile_loads = []
    for k in range(LOADS):
        piece = pl.ds(k * chunk, chunk)
        tile_loads.append(pltpu.make_async_copy(tiles_hbm.at[piece], tiles.at[piece], tile_sem.at[k]))
        tile_loads[-1].start()

    def device_at(distance):
        flat = lax.rem(me + distance + shards, shards)
        return flat // rep_count, lax.rem(flat, rep_count)

    def peer_at(o):
        size = 1 + 3 * (o // 2)
        return device_at(size * (1 - 2 * lax.rem(o, 2)))

    barrier = pltpu.get_barrier_semaphore()

    def greet(k, carry):
        pl.semaphore_signal(barrier, inc=1, device_id=device_at(k), device_id_type=MESH)
        return carry

    lax.fori_loop(1, shards, greet, 0)

    def sent(o, j):
        return rows_ref[0, o, j]

    turns = []
    for b in range(nblocks):
        turn = jnp.int32(4)
        for g in reversed(range(4)):
            hit = sent((g + 2) % 4, 0) == b
            for j in range(1, slots):
                hit = hit | (sent((g + 2) % 4, j) == b)
            turn = jnp.where(hit, g, turn)
        turns.append(turn * nblocks + b)
    places = []
    for b in range(nblocks):
        at = jnp.int32(0)
        for c in range(nblocks):
            if c != b:
                at = at + jnp.where(turns[c] < turns[b], 1, 0)
        places.append(at)
        place[b] = at
    for b in range(4 * slots):
        place[nblocks + b] = jnp.int32(nblocks + b)
    for k in range(nblocks):
        row = jnp.int32(0)
        for b in range(nblocks):
            row = row + jnp.where(places[b] == k, b, 0)
        order[k] = row

    pl.semaphore_wait(barrier, shards - 1)

    def halo_copy(it, h, o):
        at = (it * halves + h) * 4 + o
        return pltpu.make_async_remote_copy(
            src_ref=sends[it][h].at[pl.ds(o * slots, slots)],
            dst_ref=tables[it][h].at[pl.ds(nblocks + o * slots, slots)],
            send_sem=send_sem.at[at],
            recv_sem=recv_sem.at[at],
            device_id=peer_at(o),
            device_id_type=MESH,
        )

    def send_halo(it, h, o, source):
        for j in range(slots):
            row = rows_ref[0, o, j]
            sends[it][h][o * slots + j] = source[place[row] if it else row]
        halo_copy(it, h, o).start()

    def mass_copy(it, h, k):
        at = it * halves + h
        return pltpu.make_async_remote_copy(
            src_ref=mine[it][h],
            dst_ref=got[it][h].at[k - 1],
            send_sem=mass_send.at[at, k - 1],
            recv_sem=mass_recv.at[at, k - 1],
            device_id=device_at(k),
            device_id_type=MESH,
        )

    def each_other(it, h, act):
        def one(k, carry):
            act(mass_copy(it, h, k))
            return carry

        lax.fori_loop(1, shards, one, 0)

    def mass_first(it, h, mass):
        mine[it][h][...] = mass
        each_other(it, h, lambda copy: copy.start())

    def mass_total(it, h):
        each_other(it, h, lambda copy: copy.wait_recv())
        total = mine[it][h][...] + jnp.sum(got[it][h][...], axis=0)
        return 1.0 / jnp.sqrt(0.05 + total / vertices)

    def propagate(it, h, gain):
        table = tables[it][h]
        last = it + 1 == ITERS

        def row(k, mass):
            r = k if last else order[k]
            first = r * per_row
            slot = lambda t: cols_ref[first + t]
            source = slot if it == 0 else lambda t: place[slot(t)]
            left = jnp.concatenate([tiles[first + t] for t in range(per_row)], axis=1)
            right = jnp.concatenate([table[source(t)] for t in range(per_row)], axis=0)
            total = jnp.dot(left, right, preferred_element_type=jnp.float32)
            blended = gain * total + 0.1 * feats[h][r].astype(jnp.float32)
            if last:
                finals[h][k] = blended
            else:
                rounded = blended.astype(jnp.bfloat16)
                owns[h][k] = rounded
                tables[it + 1][h][k] = rounded
            squares = (blended * blended).reshape(tile_size // 8, 8, LANES)
            return mass + jnp.sum(squares, axis=0)

        def group(g, mass):
            for k in range(nblocks // 4):
                mass = row(g * (nblocks // 4) + k, mass)
            if not last:
                send_halo(it + 1, h, lax.rem(g + 2, 4), owns[h])
            return mass

        mass = lax.fori_loop(0, 4, group, jnp.zeros((8, LANES), jnp.float32))
        return jnp.sum(mass, axis=0, keepdims=True)

    for h in range(halves):
        own_loads[h].wait()
        for o in (2, 3, 0, 1):
            send_halo(0, h, o, feats[h])
    for h in range(halves):
        table_loads[h].wait()
    for load in tile_loads:
        load.wait()

    def finish(h):
        scale = mass_total(ITERS - 1, h)
        for b in range(nblocks):
            stages[h][b] = (finals[h][b] * scale).astype(jnp.bfloat16)
        pltpu.make_async_copy(
            stages[h], out_hbm.at[:, :, pl.ds(h * LANES, LANES)], out_sem.at[h]
        ).start()

    for it in range(ITERS):
        for h in range(halves):
            for o in range(4):
                halo_copy(it, h, o).wait_recv()
            gain = 0.9 if it == 0 else 0.9 * mass_total(it - 1, h)
            mass = propagate(it, h, gain)
            mass_first(it, h, mass)
    for h in range(halves):
        finish(h)
    for it in range(ITERS):
        for h in range(halves):
            for o in range(4):
                halo_copy(it, h, o).wait_send()
            each_other(it, h, lambda copy: copy.wait_send())
    for h in range(halves):
        pltpu.make_async_copy(
            stages[h], out_hbm.at[:, :, pl.ds(h * LANES, LANES)], out_sem.at[h]
        ).wait()


def local(vp_count, rep_count, features, tile_values, tile_cols, halo_rows):
    tile_size = tile_values.shape[1]
    rows, classes = features.shape
    nblocks = rows // tile_size
    slots = halo_rows.shape[2]
    halves = classes // LANES
    shards = vp_count * rep_count
    block = (tile_size, LANES)
    bf16, f32 = jnp.bfloat16, jnp.float32
    each = ITERS * halves
    scratch = [pltpu.VMEM(tile_values.shape, bf16)]
    scratch += [pltpu.VMEM((nblocks + 4 * slots,) + block, bf16)] * each
    scratch += [pltpu.VMEM((nblocks,) + block, bf16)] * (2 * halves)
    scratch += [pltpu.VMEM((4 * slots,) + block, bf16)] * each
    scratch += [pltpu.VMEM((nblocks,) + block, f32)] * halves
    scratch += [pltpu.VMEM((nblocks,) + block, bf16)] * halves
    scratch += [pltpu.VMEM((1, LANES), f32)] * each
    scratch += [pltpu.VMEM((shards - 1, 1, LANES), f32)] * each
    scratch += [pltpu.SMEM((nblocks,), jnp.int32), pltpu.SMEM((nblocks + 4 * slots,), jnp.int32)]
    dma = lambda *shape: pltpu.SemaphoreType.DMA(shape)
    scratch += [dma(LOADS), dma(halves), dma(halves), dma(halves), dma(each * 4), dma(each * 4)]
    scratch += [dma(each, shards - 1)] * 2
    out = pl.pallas_call(
        functools.partial(kernel, vp_count, rep_count, rows * shards, slots, halves),
        out_shape=jax.ShapeDtypeStruct((nblocks, tile_size, classes), bf16),
        in_specs=[pl.BlockSpec(memory_space=pltpu.SMEM)] * 2
        + [pl.BlockSpec(memory_space=pl.ANY)] * 2,
        out_specs=pl.BlockSpec(memory_space=pl.ANY),
        scratch_shapes=scratch,
        compiler_params=pltpu.CompilerParams(
            collective_id=0, has_side_effects=True, vmem_limit_bytes=60 * 1024 * 1024
        ),
    )(tile_cols, halo_rows, features.reshape(nblocks, tile_size, classes), tile_values)
    return out.reshape(rows, classes)


def solution(mesh):
    return jax.shard_map(
        functools.partial(local, mesh.shape["vp"], mesh.shape["rep"]),
        mesh=mesh,
        in_specs=(
            P(("vp", "rep"), None),
            P(("vp", "rep"), None, None),
            P(("vp", "rep")),
            P(("vp", "rep"), None, None),
        ),
        out_specs=P(("vp", "rep"), None),
        check_vma=False,
    )
```

```python
import functools

import jax
import jax.numpy as jnp
from jax import lax
from jax.experimental import pallas as pl
from jax.experimental.pallas import tpu as pltpu
from jax.sharding import PartitionSpec as P

ITERS = 3
LANES = 128
MESH = pl.DeviceIdType.MESH
LOADS = 8
UNROLL = 64


def kernel(vp_count, rep_count, vertices, slots, halves, *refs):
    cols_ref, rows_ref, feat_hbm, tiles_hbm, out_hbm = refs[:5]
    it_refs = iter(refs[5:])
    take = lambda count: [next(it_refs) for _ in range(count)]
    tiles = take(1)[0]
    tables = [take(halves) for _ in range(ITERS)]
    feats = take(halves)
    owns = take(halves)
    sends = [take(halves) for _ in range(ITERS)]
    finals = take(halves)
    stages = take(halves)
    mine = [take(halves) for _ in range(ITERS)]
    got = [take(halves) for _ in range(ITERS)]
    order, place = take(2)
    (tile_sem, feat_sem, table_sem, out_sem, send_sem, recv_sem, mass_send, mass_recv) = take(8)

    nblocks, tile_size = feats[0].shape[0], feats[0].shape[1]
    ntiles = tiles.shape[0]
    per_row = ntiles // nblocks
    my_vp, my_rep = lax.axis_index("vp"), lax.axis_index("rep")
    me = my_vp * rep_count + my_rep
    shards = vp_count * rep_count

    own_loads, table_loads = [], []
    for h in range(halves):
        part = feat_hbm.at[:, :, pl.ds(h * LANES, LANES)]
        own_loads.append(pltpu.make_async_copy(part, feats[h], feat_sem.at[h]))
        table_loads.append(
            pltpu.make_async_copy(part, tables[0][h].at[pl.ds(0, nblocks)], table_sem.at[h])
        )
    for h in range(halves):
        own_loads[h].start()
    for h in range(halves):
        table_loads[h].start()
    chunk = ntiles // LOADS
    tile_loads = []
    for k in range(LOADS):
        piece = pl.ds(k * chunk, chunk)
        tile_loads.append(pltpu.make_async_copy(tiles_hbm.at[piece], tiles.at[piece], tile_sem.at[k]))
        tile_loads[-1].start()

    def device_at(distance):
        flat = lax.rem(me + distance + shards, shards)
        return flat // rep_count, lax.rem(flat, rep_count)

    def peer_at(o):
        size = 1 + 3 * (o // 2)
        return device_at(size * (1 - 2 * lax.rem(o, 2)))

    barrier = pltpu.get_barrier_semaphore()

    def greet(k, carry):
        pl.semaphore_signal(barrier, inc=1, device_id=device_at(k), device_id_type=MESH)
        return carry

    lax.fori_loop(1, shards, greet, 0)

    def sent(o, j):
        return rows_ref[0, o, j]

    turns = []
    for b in range(nblocks):
        turn = jnp.int32(4)
        for g in reversed(range(4)):
            hit = sent((g + 2) % 4, 0) == b
            for j in range(1, slots):
                hit = hit | (sent((g + 2) % 4, j) == b)
            turn = jnp.where(hit, g, turn)
        turns.append(turn * nblocks + b)
    places = []
    for b in range(nblocks):
        at = jnp.int32(0)
        for c in range(nblocks):
            if c != b:
                at = at + jnp.where(turns[c] < turns[b], 1, 0)
        places.append(at)
        place[b] = at
    for b in range(4 * slots):
        place[nblocks + b] = jnp.int32(nblocks + b)
    for k in range(nblocks):
        row = jnp.int32(0)
        for b in range(nblocks):
            row = row + jnp.where(places[b] == k, b, 0)
        order[k] = row

    pl.semaphore_wait(barrier, shards - 1)

    def halo_copy(it, h, o):
        at = (it * halves + h) * 4 + o
        return pltpu.make_async_remote_copy(
            src_ref=sends[it][h].at[pl.ds(o * slots, slots)],
            dst_ref=tables[it][h].at[pl.ds(nblocks + o * slots, slots)],
            send_sem=send_sem.at[at],
            recv_sem=recv_sem.at[at],
            device_id=peer_at(o),
            device_id_type=MESH,
        )

    def send_halo(it, h, o, source):
        for j in range(slots):
            row = rows_ref[0, o, j]
            sends[it][h][o * slots + j] = source[place[row] if it else row]
        halo_copy(it, h, o).start()

    def mass_copy(it, h, k):
        at = it * halves + h
        return pltpu.make_async_remote_copy(
            src_ref=mine[it][h],
            dst_ref=got[it][h].at[k - 1],
            send_sem=mass_send.at[at, k - 1],
            recv_sem=mass_recv.at[at, k - 1],
            device_id=device_at(k),
            device_id_type=MESH,
        )

    def each_other(it, h, act):
        def one(k, carry):
            act(mass_copy(it, h, k))
            return carry

        lax.fori_loop(1, shards, one, 0, unroll=shards <= UNROLL)

    def mass_first(it, h, mass):
        mine[it][h][...] = mass
        each_other(it, h, lambda copy: copy.start())

    def mass_total(it, h):
        each_other(it, h, lambda copy: copy.wait_recv())
        total = mine[it][h][...] + jnp.sum(got[it][h][...], axis=0)
        return 1.0 / jnp.sqrt(0.05 + total / vertices)

    def propagate(it, h, gain):
        table = tables[it][h]
        last = it + 1 == ITERS

        def row(k, mass):
            r = k if last else order[k]
            first = r * per_row
            slot = lambda t: cols_ref[first + t]
            source = slot if it == 0 else lambda t: place[slot(t)]
            left = jnp.concatenate([tiles[first + t] for t in range(per_row)], axis=1)
            right = jnp.concatenate([table[source(t)] for t in range(per_row)], axis=0)
            total = jnp.dot(left, right, preferred_element_type=jnp.float32)
            blended = gain * total + 0.1 * feats[h][r].astype(jnp.float32)
            if last:
                finals[h][k] = blended
            else:
                rounded = blended.astype(jnp.bfloat16)
                owns[h][k] = rounded
                tables[it + 1][h][k] = rounded
            squares = (blended * blended).reshape(tile_size // 8, 8, LANES)
            return mass + jnp.sum(squares, axis=0)

        def group(g, mass):
            for k in range(nblocks // 4):
                mass = row(g * (nblocks // 4) + k, mass)
            if not last:
                send_halo(it + 1, h, lax.rem(g + 2, 4), owns[h])
            return mass

        mass = lax.fori_loop(0, 4, group, jnp.zeros((8, LANES), jnp.float32))
        return jnp.sum(mass, axis=0, keepdims=True)

    for h in range(halves):
        own_loads[h].wait()
        for o in (2, 3, 0, 1):
            send_halo(0, h, o, feats[h])
    for h in range(halves):
        table_loads[h].wait()
    for load in tile_loads:
        load.wait()

    def finish(h):
        scale = mass_total(ITERS - 1, h)
        for b in range(nblocks):
            stages[h][b] = (finals[h][b] * scale).astype(jnp.bfloat16)
        pltpu.make_async_copy(
            stages[h], out_hbm.at[:, :, pl.ds(h * LANES, LANES)], out_sem.at[h]
        ).start()

    for it in range(ITERS):
        for h in range(halves):
            for o in range(4):
                halo_copy(it, h, o).wait_recv()
            gain = 0.9 if it == 0 else 0.9 * mass_total(it - 1, h)
            mass = propagate(it, h, gain)
            mass_first(it, h, mass)
    for h in range(halves):
        finish(h)
    for it in range(ITERS):
        for h in range(halves):
            for o in range(4):
                halo_copy(it, h, o).wait_send()
            each_other(it, h, lambda copy: copy.wait_send())
    for h in range(halves):
        pltpu.make_async_copy(
            stages[h], out_hbm.at[:, :, pl.ds(h * LANES, LANES)], out_sem.at[h]
        ).wait()


def local(vp_count, rep_count, features, tile_values, tile_cols, halo_rows):
    tile_size = tile_values.shape[1]
    rows, classes = features.shape
    nblocks = rows // tile_size
    slots = halo_rows.shape[2]
    halves = classes // LANES
    shards = vp_count * rep_count
    block = (tile_size, LANES)
    bf16, f32 = jnp.bfloat16, jnp.float32
    each = ITERS * halves
    scratch = [pltpu.VMEM(tile_values.shape, bf16)]
    scratch += [pltpu.VMEM((nblocks + 4 * slots,) + block, bf16)] * each
    scratch += [pltpu.VMEM((nblocks,) + block, bf16)] * (2 * halves)
    scratch += [pltpu.VMEM((4 * slots,) + block, bf16)] * each
    scratch += [pltpu.VMEM((nblocks,) + block, f32)] * halves
    scratch += [pltpu.VMEM((nblocks,) + block, bf16)] * halves
    scratch += [pltpu.VMEM((1, LANES), f32)] * each
    scratch += [pltpu.VMEM((shards - 1, 1, LANES), f32)] * each
    scratch += [pltpu.SMEM((nblocks,), jnp.int32), pltpu.SMEM((nblocks + 4 * slots,), jnp.int32)]
    dma = lambda *shape: pltpu.SemaphoreType.DMA(shape)
    scratch += [dma(LOADS), dma(halves), dma(halves), dma(halves), dma(each * 4), dma(each * 4)]
    scratch += [dma(each, shards - 1)] * 2
    out = pl.pallas_call(
        functools.partial(kernel, vp_count, rep_count, rows * shards, slots, halves),
        out_shape=jax.ShapeDtypeStruct((nblocks, tile_size, classes), bf16),
        in_specs=[pl.BlockSpec(memory_space=pltpu.SMEM)] * 2
        + [pl.BlockSpec(memory_space=pl.ANY)] * 2,
        out_specs=pl.BlockSpec(memory_space=pl.ANY),
        scratch_shapes=scratch,
        compiler_params=pltpu.CompilerParams(
            collective_id=0, has_side_effects=True, vmem_limit_bytes=60 * 1024 * 1024
        ),
    )(tile_cols, halo_rows, features.reshape(nblocks, tile_size, classes), tile_values)
    return out.reshape(rows, classes)


def solution(mesh):
    return jax.shard_map(
        functools.partial(local, mesh.shape["vp"], mesh.shape["rep"]),
        mesh=mesh,
        in_specs=(
            P(("vp", "rep"), None),
            P(("vp", "rep"), None, None),
            P(("vp", "rep")),
            P(("vp", "rep"), None, None),
        ),
        out_specs=P(("vp", "rep"), None),
        check_vma=False,
    )
```
